32 devices in a mesh: dp: 4 (over y, x), seq: 2 (over core), head: 4 (over z).
Axes of the slice: x: 2, y: 2, z: 4, core: 2. Of those that a mesh axis runs over, the one named last changes fastest.
Arguments:
- q_lat: bfloat16 [3072, 8192], P(('dp', 'seq'), 'head'), may hold values from -160 to 160
- q_rope: bfloat16 [3072, 1024], P(('dp', 'seq'), 'head'), may hold values from -6 to 6
- grad_out: bfloat16 [3072, 8192], P(('dp', 'seq'), 'head'), may hold values from -6 to 6
- prefix_keys: bfloat16 [576, 512], P(None, 'seq'), may hold values from -6 to 6
- comp_lengths: int32 [3], replicated, may hold values from 128 to 1024, as said below
- prefix_len: int32 [1], replicated, may hold values from 65 to 512
Outputs:
- dq_lat: bfloat16 [3072, 8192], P(('dp', 'seq'), 'head')
- dq_rope: bfloat16 [3072, 1024], P(('dp', 'seq'), 'head')
- d_keys: float32 [576, 512], P(None, ('seq', 'head'))
The draws below stay inside these ranges and needn't reach their ends.
Inputs may be any that keep to these rules, and one draw needn't show every extreme that they name: `comp_lengths`: each a multiple of 128.
All inputs are finite; a program needn't handle non-finite values.
Results may differ from the reference program's by a relative error of at most 0.0089.
Values may be sent and summed in bfloat16 or wider, within the bound.
A program may use at most 64 MiB of HBM per device.

```python
import jax
import jax.numpy as jnp
from jax import lax

H = 16
DL = 512
DR = 64
CLEN = 1024
LBLK = 128
TOKENS = 3072
P_SIZE = 512
COMPS = 3


def key_matrix(key):
    values = jax.random.normal(jax.random.fold_in(key, 7001), (DL + DR, P_SIZE), jnp.float32)
    return jnp.clip(values, -6.0, 6.0)


def draw_prefix_keys(key, part):
    return key_matrix(key).astype(jnp.bfloat16)


def draw_q_lat(key, part):
    drawn = jnp.clip(jax.random.normal(jax.random.fold_in(key, 7002), (TOKENS, H * DL), jnp.float32), -6.0, 6.0)
    return jnp.clip(drawn, -160.0, 160.0).astype(jnp.bfloat16)


def draw_comp_lengths(key, part):
    counts = CLEN // LBLK
    blocks = jax.random.randint(jax.random.fold_in(key, 7011), (COMPS,), 1, counts + 1)
    offset = jax.random.randint(jax.random.fold_in(key, 7012), (), 1, counts)
    other = (blocks[0] - 1 + offset) % counts + 1
    places = jnp.arange(COMPS, dtype=jnp.int32)
    blocks = jnp.where(places == 1, other, blocks)
    return (blocks * LBLK).astype(jnp.int32)


def steps_of(stream_key, dims, split, smallest, high):
    loudness = 1.0
    for position, shards_of in split:
        draws = jax.random.uniform(jax.random.fold_in(jax.random.fold_in(stream_key, 6), position), (shards_of,), jnp.float32, smallest / len(split), high / len(split))
        loudness = loudness * jnp.repeat(jnp.exp(draws), dims[position] // shards_of).reshape((-1,) + (1,) * (len(dims) - 1 - position))
    return loudness


def normal_values(stream_key, shape, deviation, limit, cuts=(), kind=jnp.bfloat16):
    level = steps_of(stream_key, shape, cuts, -0.22, 0.18) if cuts else 1.0
    result = jax.random.normal(stream_key, shape, jnp.float32) * deviation * level
    return jnp.minimum(jnp.maximum(result, -limit), limit).astype(kind)


def setup_inputs(seed: int = 0) -> dict:
    keys = jax.random.split(jax.random.key(seed), 7)
    return {
        "q_lat": draw_q_lat(jax.random.fold_in(keys[6], 71), 0),
        "q_rope": normal_values(keys[1], (TOKENS, H * DR), 1.0, 6.0, ((0, 8), (1, 4))),
        "grad_out": normal_values(keys[2], (TOKENS, H * DL), 1.0, 6.0, ((0, 8), (1, 4))),
        "prefix_keys": draw_prefix_keys(jax.random.fold_in(keys[6], 71), 0),
        "comp_lengths": draw_comp_lengths(jax.random.fold_in(keys[6], 71), 0),
        "prefix_len": jax.random.randint(keys[5], (1,), P_SIZE // 8 + 1, P_SIZE + 1).astype(jnp.int32),
    }


def reference(q_lat, q_rope, grad_out, prefix_keys, comp_lengths, prefix_len):
    scale = (DL + DR) ** -0.5
    tok_ids = jnp.arange(TOKENS, dtype=jnp.int32)
    length = comp_lengths[(tok_ids // CLEN).astype(jnp.int32)]
    valid = (tok_ids % CLEN) < length
    keep = jnp.arange(P_SIZE, dtype=jnp.int32) < prefix_len[0]
    key_lat = prefix_keys[:DL]
    key_rope = prefix_keys[DL:]
    upstream = jnp.where(valid[:, None], grad_out, jnp.zeros_like(grad_out))
    lat_heads = q_lat.reshape(TOKENS, H, DL).transpose(1, 0, 2)
    rope_heads = q_rope.reshape(TOKENS, H, DR).transpose(1, 0, 2)
    grad_heads = upstream.reshape(TOKENS, H, DL).transpose(1, 0, 2)
    contract_last = (((1,), (1,)), ((), ()))
    contract_first = (((0,), (0,)), ((), ()))

    def head_step(carry, inputs):
        query_lat, query_rope, upgrad = inputs
        scores = (jnp.dot(query_lat, key_lat, preferred_element_type=jnp.float32)
                  + jnp.dot(query_rope, key_rope, preferred_element_type=jnp.float32)) * scale
        scores = jnp.where(keep[None, :], scores, -jnp.inf)
        peak = jnp.max(scores, axis=1, keepdims=True)
        expo = jnp.exp(scores - peak)
        prob = expo / jnp.sum(expo, axis=1, keepdims=True)
        dprob = jnp.dot(upgrad, key_lat, preferred_element_type=jnp.float32)
        delta = jnp.sum(prob * dprob, axis=1, keepdims=True)
        dscore = prob * (dprob - delta)
        prob_b = prob.astype(jnp.bfloat16)
        dscore_b = dscore.astype(jnp.bfloat16)
        grad_lat = (scale * lax.dot_general(dscore_b, key_lat, contract_last, preferred_element_type=jnp.float32)).astype(jnp.bfloat16)
        grad_rope = (scale * lax.dot_general(dscore_b, key_rope, contract_last, preferred_element_type=jnp.float32)).astype(jnp.bfloat16)
        term_lat = (lax.dot_general(upgrad, prob_b, contract_first, preferred_element_type=jnp.float32)
                    + scale * lax.dot_general(query_lat, dscore_b, contract_first, preferred_element_type=jnp.float32))
        term_rope = scale * lax.dot_general(query_rope, dscore_b, contract_first, preferred_element_type=jnp.float32)
        carry = carry + jnp.concatenate([term_lat, term_rope], axis=0)
        return carry, (grad_lat, grad_rope)

    start = jnp.zeros((DL + DR, P_SIZE), jnp.float32)
    key_grads, outputs = lax.scan(head_step, start, (lat_heads, rope_heads, grad_heads))
    dq_lat = outputs[0].transpose(1, 0, 2).reshape(TOKENS, H * DL)
    dq_rope = outputs[1].transpose(1, 0, 2).reshape(TOKENS, H * DR)
    return (dq_lat, dq_rope, key_grads)
```

```python
import functools

import jax
import jax.numpy as jnp
from jax import lax
from jax.experimental import pallas as pl
from jax.experimental.pallas import tpu as pltpu
from jax.sharding import PartitionSpec as P

DL = 512
DR = 64
CLEN = 1024
MESH = pl.DeviceIdType.MESH
NEG = -1e30
F32 = jnp.float32
BF16 = jnp.bfloat16


def dot(a, b, da, db):
    return lax.dot_general(a, b, (((da,), (db,)), ((), ())), preferred_element_type=F32)


def compute_kernel(tok_rows, lens_ref, plen_ref, q_ref, qr_ref, g_ref, keys_ref,
                   dq_ref, dqr_ref, terms_ref, keys_t, rope_t, acc_p, acc_q, acc_r):
    head = pl.program_id(0)
    parity = lax.rem(head, 2)
    scale = (DL + DR) ** (-0.5)
    cols = keys_ref.shape[1]

    @pl.when(head == 0)
    def _():
        keys_t[...] = keys_ref[:DL].T
        rope = keys_ref[DL:].astype(F32).T
        zero = jnp.zeros_like(rope)
        rope_t[0] = jnp.concatenate([rope, zero], axis=1).astype(BF16)
        rope_t[1] = jnp.concatenate([zero, rope], axis=1).astype(BF16)
        acc_p[...] = jnp.zeros_like(acc_p)
        acc_q[...] = jnp.zeros_like(acc_q)
        acc_r[...] = jnp.zeros_like(acc_r)

    first = (lax.axis_index("dp") * lax.axis_size("seq") + lax.axis_index("seq")) * tok_rows
    tok = first + lax.broadcasted_iota(jnp.int32, (tok_rows, 1), 0)
    comp = tok // CLEN
    length = jnp.zeros_like(tok)
    for c in range(lens_ref.shape[0]):
        length = jnp.where(comp == c, lens_ref[c], length)
    valid = tok - comp * CLEN < length
    g = jnp.where(valid, g_ref[...].astype(F32), 0.0).astype(BF16)
    q = q_ref[...]
    qr = qr_ref[...]
    kt = keys_t[...]
    rt = rope_t[parity]
    s = (dot(kt, q, 1, 1) + dot(rt, qr, 1, 1)) * scale
    keep = lax.broadcasted_iota(jnp.int32, (cols, 1), 0) < plen_ref[0]
    s = jnp.where(keep, s, NEG)
    e = jnp.exp(s - jnp.max(s, axis=0, keepdims=True))
    inv = 1.0 / jnp.sum(e, axis=0, keepdims=True)
    dp = dot(kt, g, 1, 1)
    p = e * inv
    delta = jnp.sum(p * dp, axis=0, keepdims=True)
    ds = (p * (dp - delta)).astype(BF16)
    acc_p[...] += dot(p.astype(BF16), g, 1, 0)
    acc_q[...] += dot(ds, q, 1, 0)
    acc_r[parity] += dot(ds, qr, 1, 0)
    dst = ds.T
    dq_ref[...] = (scale * dot(dst, kt, 1, 0)).astype(BF16)
    half = (scale * dot(dst, rt, 1, 0)).astype(BF16)

    @pl.when(parity == 0)
    def _():
        dqr_ref[...] = half

    @pl.when(parity == 1)
    def _():
        dqr_ref[...] += half

    @pl.when(head == pl.num_programs(0) - 1)
    def _():
        terms_ref[:, :DL] = (acc_p[...] + scale * acc_q[...]).astype(BF16)
        terms_ref[:, DL:] = (scale * (acc_r[0][:, :DR] + acc_r[1][:, DR:])).astype(BF16)


def compute(q_lat, q_rope, grad_out, keys, comp_lengths, prefix_len):
    tok_rows = q_lat.shape[0]
    heads = q_lat.shape[1] // DL
    cols = keys.shape[1]
    lat = pl.BlockSpec((tok_rows, DL), lambda h: (0, h))
    rope = pl.BlockSpec((tok_rows, 2 * DR), lambda h: (0, h // 2))
    smem = pl.BlockSpec(memory_space=pltpu.SMEM)
    return pl.pallas_call(
        functools.partial(compute_kernel, tok_rows),
        grid=(heads,),
        out_shape=(
            jax.ShapeDtypeStruct(q_lat.shape, BF16),
            jax.ShapeDtypeStruct(q_rope.shape, BF16),
            jax.ShapeDtypeStruct((cols, DL + DR), BF16),
        ),
        in_specs=[smem, smem, lat, rope, lat, pl.BlockSpec((DL + DR, cols), lambda h: (0, 0))],
        out_specs=(lat, rope, pl.BlockSpec((cols, DL + DR), lambda h: (0, 0))),
        scratch_shapes=[
            pltpu.VMEM((cols, DL), BF16),
            pltpu.VMEM((2, cols, 2 * DR), BF16),
            pltpu.VMEM((cols, DL), F32),
            pltpu.VMEM((cols, DL), F32),
            pltpu.VMEM((2, cols, 2 * DR), F32),
        ],
        compiler_params=pltpu.CompilerParams(
            dimension_semantics=("arbitrary",), vmem_limit_bytes=60 * 1024 * 1024
        ),
        name="attend",
    )(comp_lengths, prefix_len, q_lat, q_rope, grad_out, keys)


def reduce_kernel(ns, nd, nh, x_ref, o_ref, r1, y, r2, z, r3, u, sends, recvs):
    me_s = lax.axis_index("seq")
    me_d = lax.axis_index("dp")
    me_h = lax.axis_index("head")
    barrier = pltpu.get_barrier_semaphore()
    for axis, me, n in (("seq", me_s, ns), ("dp", me_d, nd), ("head", me_h, nh)):
        for off in range(1, n):
            pl.semaphore_signal(
                barrier, inc=1, device_id={axis: lax.rem(me + off, n)}, device_id_type=MESH
            )
    pl.semaphore_wait(barrier, ns + nd + nh - 3)

    count = [0]

    def exchange(axis, me, n, source, target):
        copies = []
        for off in range(1, n):
            peer = lax.rem(me + off, n)
            k = count[0]
            count[0] += 1
            copy = pltpu.make_async_remote_copy(
                src_ref=source(peer), dst_ref=target(off), send_sem=sends.at[k],
                recv_sem=recvs.at[k], device_id={axis: peer}, device_id_type=MESH,
            )
            copy.start()
            copies.append(copy)
        return copies

    pending = []
    copies = exchange("seq", me_s, ns, lambda p: x_ref.at[p], lambda off: r1.at[off - 1])
    total = x_ref[me_s].astype(F32)
    for off, copy in enumerate(copies):
        copy.wait_recv()
        total += r1[off].astype(F32)
    y[...] = total.astype(BF16)
    pending += copies

    copies = exchange("dp", me_d, nd, lambda p: y.at[:, p], lambda off: r2.at[off - 1])
    total = y[:, me_d].astype(F32)
    for off, copy in enumerate(copies):
        copy.wait_recv()
        total += r2[off].astype(F32)
    z[...] = total.astype(BF16)
    pending += copies

    copies = exchange("head", me_h, nh, lambda p: z.at[p], lambda off: r3.at[off - 1])
    total = z[me_h].astype(F32)
    for off, copy in enumerate(copies):
        copy.wait_recv()
        total += r3[off].astype(F32)
    u[...] = total.astype(BF16)
    pending += copies

    copies = exchange("dp", me_d, nd, lambda p: u, lambda off: o_ref.at[me_d])
    o_ref[me_d] = u[...]
    for copy in copies:
        copy.wait_recv()
    pending += copies
    for copy in pending:
        copy.wait_send()


def reduce_terms(terms):
    ns, nd, nh = (lax.axis_size(a) for a in ("seq", "dp", "head"))
    width = terms.shape[1]
    part = terms.shape[0] // (ns * nh * nd)
    x = terms.reshape(ns, nh, nd, part, width)
    total = ns + 2 * nd + nh - 4
    vmem = pl.BlockSpec(memory_space=pltpu.VMEM)
    out = pl.pallas_call(
        functools.partial(reduce_kernel, ns, nd, nh),
        out_shape=jax.ShapeDtypeStruct((nd, part, width), BF16),
        in_specs=[vmem],
        out_specs=vmem,
        scratch_shapes=[
            pltpu.VMEM((ns - 1, nh, nd, part, width), BF16),
            pltpu.VMEM((nh, nd, part, width), BF16),
            pltpu.VMEM((nd - 1, nh, part, width), BF16),
            pltpu.VMEM((nh, part, width), BF16),
            pltpu.VMEM((nh - 1, part, width), BF16),
            pltpu.VMEM((part, width), BF16),
            pltpu.SemaphoreType.DMA((total,)),
            pltpu.SemaphoreType.DMA((total,)),
        ],
        compiler_params=pltpu.CompilerParams(collective_id=0, has_side_effects=True),
        name="reduce_keys",
    )(x)
    return out.reshape(nd * part, width).T.astype(F32)


def on_device(q_lat, q_rope, grad_out, prefix_keys, comp_lengths, prefix_len):
    keys = lax.all_gather(prefix_keys, "seq", axis=1, tiled=True)
    dq_lat, dq_rope, terms = compute(q_lat, q_rope, grad_out, keys, comp_lengths, prefix_len)
    return dq_lat, dq_rope, reduce_terms(terms)


def solution(mesh):
    in_specs = (
        P(("dp", "seq"), "head"),
        P(("dp", "seq"), "head"),
        P(("dp", "seq"), "head"),
        P(None, "seq"),
        P(),
        P(),
    )
    out_specs = (P(("dp", "seq"), "head"), P(("dp", "seq"), "head"), P(None, ("seq", "head")))
    return jax.shard_map(
        on_device, mesh=mesh, in_specs=in_specs, out_specs=out_specs, check_vma=False
    )
```

```python
import functools

import jax
import jax.numpy as jnp
from jax import lax
from jax.experimental import pallas as pl
from jax.experimental.pallas import tpu as pltpu
from jax.sharding import PartitionSpec as P

DL = 512
DR = 64
CLEN = 1024
MESH = pl.DeviceIdType.MESH
NEG = -1e30
F32 = jnp.float32
BF16 = jnp.bfloat16


def dot(a, b, da, db):
    return lax.dot_general(a, b, (((da,), (db,)), ((), ())), preferred_element_type=F32)


def head_step(used, parity, scale, g, plen_ref, q_ref, qr_ref,
              dq_ref, dqr_ref, keys_t, rope_t, acc_p, acc_q, acc_r):
    q = q_ref[...]
    qr = qr_ref[...]
    kt = keys_t[:used]
    rt = rope_t[parity, :used]
    s = (dot(kt, q, 1, 1) + dot(rt, qr, 1, 1)) * scale
    keep = lax.broadcasted_iota(jnp.int32, (used, 1), 0) < plen_ref[0]
    s = jnp.where(keep, s, NEG)
    e = jnp.exp(s - jnp.max(s, axis=0, keepdims=True))
    inv = 1.0 / jnp.sum(e, axis=0, keepdims=True)
    dp = dot(kt, g, 1, 1)
    p = e * inv
    delta = jnp.sum(p * dp, axis=0, keepdims=True)
    ds = (p * (dp - delta)).astype(BF16)
    acc_p[:used] += dot(p.astype(BF16), g, 1, 0)
    acc_q[:used] += dot(ds, q, 1, 0)
    acc_r[parity, :used] += dot(ds, qr, 1, 0)
    dst = ds.T
    dq_ref[...] = (scale * dot(dst, kt, 1, 0)).astype(BF16)
    half = (scale * dot(dst, rt, 1, 0)).astype(BF16)

    @pl.when(parity == 0)
    def _():
        dqr_ref[...] = half

    @pl.when(parity == 1)
    def _():
        dqr_ref[...] += half


def compute_kernel(tok_rows, lens_ref, plen_ref, q_ref, qr_ref, g_ref, keys_ref,
                   dq_ref, dqr_ref, terms_ref, keys_t, rope_t, acc_p, acc_q, acc_r):
    head = pl.program_id(0)
    parity = lax.rem(head, 2)
    scale = (DL + DR) ** (-0.5)
    parts, _, wide = keys_ref.shape
    cols = parts * wide

    @pl.when(head == 0)
    def _():
        for part in range(parts):
            rows = pl.ds(part * wide, wide)
            keys_t[rows] = keys_ref[part, :DL].T
            rope = keys_ref[part, DL:].astype(F32).T
            zero = jnp.zeros_like(rope)
            rope_t[0, rows] = jnp.concatenate([rope, zero], axis=1).astype(BF16)
            rope_t[1, rows] = jnp.concatenate([zero, rope], axis=1).astype(BF16)
        acc_p[...] = jnp.zeros_like(acc_p)
        acc_q[...] = jnp.zeros_like(acc_q)
        acc_r[...] = jnp.zeros_like(acc_r)

    first = (lax.axis_index("dp") * lax.axis_size("seq") + lax.axis_index("seq")) * tok_rows
    tok = first + lax.broadcasted_iota(jnp.int32, (tok_rows, 1), 0)
    comp = tok // CLEN
    length = jnp.zeros_like(tok)
    for c in range(lens_ref.shape[0]):
        length = jnp.where(comp == c, lens_ref[c], length)
    valid = tok - comp * CLEN < length
    g = jnp.where(valid, g_ref[...].astype(F32), 0.0).astype(BF16)
    step = cols // 4 if cols % 512 == 0 else cols
    blocks = (plen_ref[0] + step - 1) // step

    for used in range(step, cols + 1, step):

        @pl.when(blocks == used // step)
        def _():
            head_step(used, parity, scale, g, plen_ref, q_ref, qr_ref,
                      dq_ref, dqr_ref, keys_t, rope_t, acc_p, acc_q, acc_r)

    @pl.when(head == pl.num_programs(0) - 1)
    def _():
        terms_ref[:, :DL] = (acc_p[...] + scale * acc_q[...]).astype(BF16)
        terms_ref[:, DL:] = (scale * (acc_r[0][:, :DR] + acc_r[1][:, DR:])).astype(BF16)


def compute(q_lat, q_rope, grad_out, keys, comp_lengths, prefix_len):
    tok_rows = q_lat.shape[0]
    heads = q_lat.shape[1] // DL
    cols = keys.shape[0] * keys.shape[2]
    lat = pl.BlockSpec((tok_rows, DL), lambda h: (0, h))
    rope = pl.BlockSpec((tok_rows, 2 * DR), lambda h: (0, h // 2))
    smem = pl.BlockSpec(memory_space=pltpu.SMEM)
    return pl.pallas_call(
        functools.partial(compute_kernel, tok_rows),
        grid=(heads,),
        out_shape=(
            jax.ShapeDtypeStruct(q_lat.shape, BF16),
            jax.ShapeDtypeStruct(q_rope.shape, BF16),
            jax.ShapeDtypeStruct((cols, DL + DR), BF16),
        ),
        in_specs=[smem, smem, lat, rope, lat, pl.BlockSpec(keys.shape, lambda h: (0, 0, 0))],
        out_specs=(lat, rope, pl.BlockSpec((cols, DL + DR), lambda h: (0, 0))),
        scratch_shapes=[
            pltpu.VMEM((cols, DL), BF16),
            pltpu.VMEM((2, cols, 2 * DR), BF16),
            pltpu.VMEM((cols, DL), F32),
            pltpu.VMEM((cols, DL), F32),
            pltpu.VMEM((2, cols, 2 * DR), F32),
        ],
        compiler_params=pltpu.CompilerParams(
            dimension_semantics=("arbitrary",), vmem_limit_bytes=60 * 1024 * 1024
        ),
        name="attend",
    )(comp_lengths, prefix_len, q_lat, q_rope, grad_out, keys)


def reduce_kernel(ns, nd, nh, x_ref, o_ref, r1, y, r2, z, r3, u, sends, recvs):
    me_s = lax.axis_index("seq")
    me_d = lax.axis_index("dp")
    me_h = lax.axis_index("head")
    barrier = pltpu.get_barrier_semaphore()
    for axis, me, n in (("seq", me_s, ns), ("dp", me_d, nd), ("head", me_h, nh)):
        for off in range(1, n):
            pl.semaphore_signal(
                barrier, inc=1, device_id={axis: lax.rem(me + off, n)}, device_id_type=MESH
            )
    pl.semaphore_wait(barrier, ns + nd + nh - 3)

    count = [0]

    def exchange(axis, me, n, source, target):
        copies = []
        for off in range(1, n):
            peer = lax.rem(me + off, n)
            k = count[0]
            count[0] += 1
            copy = pltpu.make_async_remote_copy(
                src_ref=source(peer), dst_ref=target(off), send_sem=sends.at[k],
                recv_sem=recvs.at[k], device_id={axis: peer}, device_id_type=MESH,
            )
            copy.start()
            copies.append(copy)
        return copies

    pending = []
    copies = exchange("seq", me_s, ns, lambda p: x_ref.at[p], lambda off: r1.at[off - 1])
    total = x_ref[me_s].astype(F32)
    for off, copy in enumerate(copies):
        copy.wait_recv()
        total += r1[off].astype(F32)
    y[...] = total.astype(BF16)
    pending += copies

    copies = exchange("dp", me_d, nd, lambda p: y.at[:, p], lambda off: r2.at[off - 1])
    total = y[:, me_d].astype(F32)
    for off, copy in enumerate(copies):
        copy.wait_recv()
        total += r2[off].astype(F32)
    z[...] = total.astype(BF16)
    pending += copies

    copies = exchange("head", me_h, nh, lambda p: z.at[p], lambda off: r3.at[off - 1])
    total = z[me_h].astype(F32)
    for off, copy in enumerate(copies):
        copy.wait_recv()
        total += r3[off].astype(F32)
    u[...] = total.astype(BF16)
    pending += copies

    copies = exchange("dp", me_d, nd, lambda p: u, lambda off: o_ref.at[me_d])
    o_ref[me_d] = u[...]
    for copy in copies:
        copy.wait_recv()
    pending += copies
    for copy in pending:
        copy.wait_send()


def widen_kernel(x_ref, o_ref):
    o_ref[...] = x_ref[...].astype(F32)


def gather_kernel(ns, x_ref, o_ref, sends, recvs):
    me = lax.axis_index("seq")
    barrier = pltpu.get_barrier_semaphore()
    peers = [lax.rem(me + off, ns) for off in range(1, ns)]
    for peer in peers:
        pl.semaphore_signal(barrier, inc=1, device_id={"seq": peer}, device_id_type=MESH)
    pl.semaphore_wait(barrier, ns - 1)
    copies = [
        pltpu.make_async_remote_copy(
            src_ref=x_ref, dst_ref=o_ref.at[me], send_sem=sends.at[k], recv_sem=recvs.at[k],
            device_id={"seq": peer}, device_id_type=MESH,
        )
        for k, peer in enumerate(peers)
    ]
    for copy in copies:
        copy.start()
    o_ref[me] = x_ref[...]
    for copy in copies:
        copy.wait()


def gather(keys):
    ns = lax.axis_size("seq")
    vmem = pl.BlockSpec(memory_space=pltpu.VMEM)
    return pl.pallas_call(
        functools.partial(gather_kernel, ns),
        out_shape=jax.ShapeDtypeStruct((ns, *keys.shape), keys.dtype),
        in_specs=[vmem],
        out_specs=vmem,
        scratch_shapes=[pltpu.SemaphoreType.DMA((ns - 1,)), pltpu.SemaphoreType.DMA((ns - 1,))],
        compiler_params=pltpu.CompilerParams(collective_id=1, has_side_effects=True),
        name="gather_keys",
    )(keys)


def reduce_terms(terms):
    ns, nd, nh = (lax.axis_size(a) for a in ("seq", "dp", "head"))
    width = terms.shape[1]
    part = terms.shape[0] // (ns * nh * nd)
    x = terms.reshape(ns, nh, nd, part, width)
    total = ns + 2 * nd + nh - 4
    vmem = pl.BlockSpec(memory_space=pltpu.VMEM)
    out = pl.pallas_call(
        functools.partial(reduce_kernel, ns, nd, nh),
        out_shape=jax.ShapeDtypeStruct((nd, part, width), BF16),
        in_specs=[vmem],
        out_specs=vmem,
        scratch_shapes=[
            pltpu.VMEM((ns - 1, nh, nd, part, width), BF16),
            pltpu.VMEM((nh, nd, part, width), BF16),
            pltpu.VMEM((nd - 1, nh, part, width), BF16),
            pltpu.VMEM((nh, part, width), BF16),
            pltpu.VMEM((nh - 1, part, width), BF16),
            pltpu.VMEM((part, width), BF16),
            pltpu.SemaphoreType.DMA((total,)),
            pltpu.SemaphoreType.DMA((total,)),
        ],
        compiler_params=pltpu.CompilerParams(collective_id=0, has_side_effects=True),
        name="reduce_keys",
    )(x)
    return pl.pallas_call(
        widen_kernel,
        out_shape=jax.ShapeDtypeStruct((nd * part, width), F32),
        in_specs=[vmem],
        out_specs=vmem,
        name="widen",
    )(out.reshape(nd * part, width)).T


def on_device(q_lat, q_rope, grad_out, prefix_keys, comp_lengths, prefix_len):
    keys = gather(prefix_keys)
    dq_lat, dq_rope, terms = compute(q_lat, q_rope, grad_out, keys, comp_lengths, prefix_len)
    return dq_lat, dq_rope, reduce_terms(terms)


def solution(mesh):
    in_specs = (
        P(("dp", "seq"), "head"),
        P(("dp", "seq"), "head"),
        P(("dp", "seq"), "head"),
        P(None, "seq"),
        P(),
        P(),
    )
    out_specs = (P(("dp", "seq"), "head"), P(("dp", "seq"), "head"), P(None, ("seq", "head")))
    return jax.shard_map(
        on_device, mesh=mesh, in_specs=in_specs, out_specs=out_specs, check_vma=False
    )
```

```python
import functools

import jax
import jax.numpy as jnp
from jax import lax
from jax.experimental import pallas as pl
from jax.experimental.pallas import tpu as pltpu
from jax.sharding import PartitionSpec as P

DL = 512
DR = 64
CLEN = 1024
MESH = pl.DeviceIdType.MESH
NEG = -1e30
F32 = jnp.float32
BF16 = jnp.bfloat16


def dot(a, b, da, db):
    return lax.dot_general(a, b, (((da,), (db,)), ((), ())), preferred_element_type=F32)


def pair_step(used, scale, g, q, qr, plen_ref, dq_ref, dqr_ref, keys_t, rope_t, acc_p, acc_q, acc_r):
    tok_rows = dq_ref.shape[0]
    kt = keys_t[:used]
    rt = rope_t[:used]
    s = (dot(kt, q, 1, 1) + dot(rt, qr, 1, 1)) * scale
    keep = lax.broadcasted_iota(jnp.int32, (used, 1), 0) < plen_ref[0]
    s = jnp.where(keep, s, NEG)
    e = jnp.exp(s - jnp.max(s, axis=0, keepdims=True))
    inv = 1.0 / jnp.sum(e, axis=0, keepdims=True)
    dp = dot(kt, g, 1, 1)
    p = e * inv
    delta = jnp.sum(p * dp, axis=0, keepdims=True)
    ds = (p * (dp - delta)).astype(BF16)
    acc_p[:used] += dot(p.astype(BF16), g, 1, 0)
    acc_q[:used] += dot(ds, q, 1, 0)
    acc_r[:used] += dot(ds, qr, 1, 0)
    dst = ds.T
    dq = (scale * dot(dst, kt, 1, 0)).astype(BF16)
    dq_ref[:, :DL] = dq[:tok_rows]
    dq_ref[:, DL:] = dq[tok_rows:]
    both = scale * dot(dst, rt, 1, 0)
    left = lax.broadcasted_iota(jnp.int32, (1, 2 * DR), 1) < DR
    dqr_ref[...] = jnp.where(left, both[:tok_rows], both[tok_rows:]).astype(BF16)


def compute_kernel(tok_rows, lens_ref, plen_ref, q_ref, qr_ref, g_ref, keys_ref,
                   dq_ref, dqr_ref, terms_ref, keys_t, rope_t, acc_p, acc_q, acc_r):
    head = pl.program_id(0)
    scale = (DL + DR) ** (-0.5)
    parts, _, wide = keys_ref.shape
    cols = parts * wide

    @pl.when(head == 0)
    def _():
        for part in range(parts):
            rows = pl.ds(part * wide, wide)
            keys_t[rows] = keys_ref[part, :DL].T
            rope = keys_ref[part, DL:].astype(F32).T
            rope_t[rows] = jnp.concatenate([rope, rope], axis=1).astype(BF16)
        acc_p[...] = jnp.zeros_like(acc_p)
        acc_q[...] = jnp.zeros_like(acc_q)
        acc_r[...] = jnp.zeros_like(acc_r)

    first = (lax.axis_index("dp") * lax.axis_size("seq") + lax.axis_index("seq")) * tok_rows
    tok = first + lax.broadcasted_iota(jnp.int32, (tok_rows, 1), 0)
    comp = tok // CLEN
    length = jnp.zeros_like(tok)
    for c in range(lens_ref.shape[0]):
        length = jnp.where(comp == c, lens_ref[c], length)
    valid = tok - comp * CLEN < length
    g = jnp.where(valid, g_ref[...].astype(F32), 0.0).astype(BF16)
    g = jnp.concatenate([g[:, :DL], g[:, DL:]], axis=0)
    q = jnp.concatenate([q_ref[:, :DL], q_ref[:, DL:]], axis=0)
    qr = qr_ref[...].astype(F32)
    left = lax.broadcasted_iota(jnp.int32, (1, 2 * DR), 1) < DR
    qr = jnp.concatenate([jnp.where(left, qr, 0.0), jnp.where(left, 0.0, qr)], axis=0).astype(BF16)
    step = cols // 4 if cols % 512 == 0 else cols
    blocks = (plen_ref[0] + step - 1) // step

    for used in range(step, cols + 1, step):

        @pl.when(blocks == used // step)
        def _():
            pair_step(used, scale, g, q, qr, plen_ref, dq_ref, dqr_ref,
                      keys_t, rope_t, acc_p, acc_q, acc_r)

    @pl.when(head == pl.num_programs(0) - 1)
    def _():
        terms_ref[:, :DL] = (acc_p[...] + scale * acc_q[...]).astype(BF16)
        terms_ref[:, DL:] = (scale * (acc_r[:, :DR] + acc_r[:, DR:])).astype(BF16)


def compute(q_lat, q_rope, grad_out, keys, comp_lengths, prefix_len):
    tok_rows = q_lat.shape[0]
    heads = q_lat.shape[1] // DL
    cols = keys.shape[0] * keys.shape[2]
    lat = pl.BlockSpec((tok_rows, 2 * DL), lambda h: (0, h))
    rope = pl.BlockSpec((tok_rows, 2 * DR), lambda h: (0, h))
    smem = pl.BlockSpec(memory_space=pltpu.SMEM)
    return pl.pallas_call(
        functools.partial(compute_kernel, tok_rows),
        grid=(heads // 2,),
        out_shape=(
            jax.ShapeDtypeStruct(q_lat.shape, BF16),
            jax.ShapeDtypeStruct(q_rope.shape, BF16),
            jax.ShapeDtypeStruct((cols, DL + DR), BF16),
        ),
        in_specs=[smem, smem, lat, rope, lat, pl.BlockSpec(keys.shape, lambda h: (0, 0, 0))],
        out_specs=(lat, rope, pl.BlockSpec((cols, DL + DR), lambda h: (0, 0))),
        scratch_shapes=[
            pltpu.VMEM((cols, DL), BF16),
            pltpu.VMEM((cols, 2 * DR), BF16),
            pltpu.VMEM((cols, DL), F32),
            pltpu.VMEM((cols, DL), F32),
            pltpu.VMEM((cols, 2 * DR), F32),
        ],
        compiler_params=pltpu.CompilerParams(
            dimension_semantics=("arbitrary",), vmem_limit_bytes=60 * 1024 * 1024
        ),
        name="attend",
    )(comp_lengths, prefix_len, q_lat, q_rope, grad_out, keys)


def reduce_kernel(ns, nd, nh, cuts, src_ref, o_ref, x_ref, r1, y, r2, z, r3, u, sends, recvs, load):
    me_s = lax.axis_index("seq")
    me_d = lax.axis_index("dp")
    me_h = lax.axis_index("head")
    copy_in = pltpu.make_async_copy(src_ref, x_ref, load)
    copy_in.start()
    barrier = pltpu.get_barrier_semaphore()
    for axis, me, n in (("seq", me_s, ns), ("dp", me_d, nd), ("head", me_h, nh)):
        for off in range(1, n):
            pl.semaphore_signal(
                barrier, inc=1, device_id={axis: lax.rem(me + off, n)}, device_id_type=MESH
            )
    copy_in.wait()
    pl.semaphore_wait(barrier, ns + nd + nh - 3)

    count = [0]
    pending = []

    def exchange(axis, me, n, source, target):
        copies = []
        for off in range(1, n):
            peer = lax.rem(me + off, n)
            k = count[0]
            count[0] += 1
            copy = pltpu.make_async_remote_copy(
                src_ref=source(peer), dst_ref=target(off), send_sem=sends.at[k],
                recv_sem=recvs.at[k], device_id={axis: peer}, device_id_type=MESH,
            )
            copy.start()
            copies.append(copy)
        pending.extend(copies)
        return copies

    def summed(own, landed, copies):
        total = own.astype(F32)
        for off, copy in enumerate(copies):
            copy.wait_recv()
            total += landed(off).astype(F32)
        return total.astype(BF16)

    lanes = [pl.ds(lo, hi - lo) for lo, hi in cuts]
    stage = [
        exchange("seq", me_s, ns, lambda p, c=c: x_ref.at[p, :, :, :, c],
                 lambda off, c=c: r1.at[off - 1, :, :, :, c])
        for c in lanes
    ]
    after = []
    for c, copies in zip(lanes, stage):
        y[:, :, :, c] = summed(x_ref[me_s, :, :, :, c], lambda off: r1[off, :, :, :, c], copies)
        after.append(exchange("dp", me_d, nd, lambda p: y.at[:, p, :, c],
                              lambda off: r2.at[off - 1, :, :, c]))
    stage, after = after, []
    for c, copies in zip(lanes, stage):
        z[:, :, c] = summed(y[:, me_d, :, c], lambda off: r2[off, :, :, c], copies)
        after.append(exchange("head", me_h, nh, lambda p: z.at[p, :, c],
                              lambda off: r3.at[off - 1, :, c]))
    stage, after = after, []
    for c, copies in zip(lanes, stage):
        u[:, c] = summed(z[me_h, :, c], lambda off: r3[off, :, c], copies)
        after.append(exchange("dp", me_d, nd, lambda p: u.at[:, c], lambda off: o_ref.at[me_d, :, c]))
    o_ref[me_d] = u[...]
    for copies in after:
        for copy in copies:
            copy.wait_recv()
    for copy in pending:
        copy.wait_send()


def widen_kernel(x_ref, o_ref):
    o_ref[...] = x_ref[...].astype(F32)


def gather_kernel(ns, x_ref, o_ref, sends, recvs):
    me = lax.axis_index("seq")
    barrier = pltpu.get_barrier_semaphore()
    peers = [lax.rem(me + off, ns) for off in range(1, ns)]
    for peer in peers:
        pl.semaphore_signal(barrier, inc=1, device_id={"seq": peer}, device_id_type=MESH)
    pl.semaphore_wait(barrier, ns - 1)
    copies = [
        pltpu.make_async_remote_copy(
            src_ref=x_ref, dst_ref=o_ref.at[me], send_sem=sends.at[k], recv_sem=recvs.at[k],
            device_id={"seq": peer}, device_id_type=MESH,
        )
        for k, peer in enumerate(peers)
    ]
    for copy in copies:
        copy.start()
    o_ref[me] = x_ref[...]
    for copy in copies:
        copy.wait()


def gather(keys):
    ns = lax.axis_size("seq")
    vmem = pl.BlockSpec(memory_space=pltpu.VMEM)
    return pl.pallas_call(
        functools.partial(gather_kernel, ns),
        out_shape=jax.ShapeDtypeStruct((ns, *keys.shape), keys.dtype),
        in_specs=[vmem],
        out_specs=vmem,
        scratch_shapes=[pltpu.SemaphoreType.DMA((ns - 1,)), pltpu.SemaphoreType.DMA((ns - 1,))],
        compiler_params=pltpu.CompilerParams(collective_id=1, has_side_effects=True),
        name="gather_keys",
    )(keys)


def reduce_terms(terms):
    ns, nd, nh = (lax.axis_size(a) for a in ("seq", "dp", "head"))
    width = terms.shape[1]
    part = terms.shape[0] // (ns * nh * nd)
    x = terms.reshape(ns, nh, nd, part, width)
    cuts = ((0, DL // 2), (DL // 2, width))
    total = (ns + 2 * nd + nh - 4) * len(cuts)
    vmem = pl.BlockSpec(memory_space=pltpu.VMEM)
    out = pl.pallas_call(
        functools.partial(reduce_kernel, ns, nd, nh, cuts),
        out_shape=jax.ShapeDtypeStruct((nd, part, width), BF16),
        in_specs=[pl.BlockSpec(memory_space=pl.ANY)],
        out_specs=vmem,
        scratch_shapes=[
            pltpu.VMEM((ns, nh, nd, part, width), BF16),
            pltpu.VMEM((ns - 1, nh, nd, part, width), BF16),
            pltpu.VMEM((nh, nd, part, width), BF16),
            pltpu.VMEM((nd - 1, nh, part, width), BF16),
            pltpu.VMEM((nh, part, width), BF16),
            pltpu.VMEM((nh - 1, part, width), BF16),
            pltpu.VMEM((part, width), BF16),
            pltpu.SemaphoreType.DMA((total,)),
            pltpu.SemaphoreType.DMA((total,)),
            pltpu.SemaphoreType.DMA,
        ],
        compiler_params=pltpu.CompilerParams(collective_id=0, has_side_effects=True),
        name="reduce_keys",
    )(x)
    return pl.pallas_call(
        widen_kernel,
        out_shape=jax.ShapeDtypeStruct((nd * part, width), F32),
        in_specs=[vmem],
        out_specs=vmem,
        name="widen",
    )(out.reshape(nd * part, width)).T


def on_device(q_lat, q_rope, grad_out, prefix_keys, comp_lengths, prefix_len):
    keys = gather(prefix_keys)
    dq_lat, dq_rope, terms = compute(q_lat, q_rope, grad_out, keys, comp_lengths, prefix_len)
    return dq_lat, dq_rope, reduce_terms(terms)


def solution(mesh):
    in_specs = (
        P(("dp", "seq"), "head"),
        P(("dp", "seq"), "head"),
        P(("dp", "seq"), "head"),
        P(None, "seq"),
        P(),
        P(),
    )
    out_specs = (P(("dp", "seq"), "head"), P(("dp", "seq"), "head"), P(None, ("seq", "head")))
    return jax.shard_map(
        on_device, mesh=mesh, in_specs=in_specs, out_specs=out_specs, check_vma=False
    )
```
